32 devices in a mesh: lat: 8 (over z, y), lon: 4 (over x, core).
Axes of the slice: x: 2, y: 2, z: 4, core: 2. Of those that a mesh axis runs over, the one named last changes fastest.
Arguments:
- x_fwd: bfloat16 [128, 384, 256], P('lat', 'lon'), may hold values from -6 to 6
- x_prev: bfloat16 [128, 384, 256], P('lat', 'lon'), may hold values from -6 to 6
- grad_out: bfloat16 [128, 384, 256], P('lat', 'lon'), may hold values from -6 to 6
- weight: bfloat16 [2048, 256], replicated, may hold values from -0.125 to 0.125
- basis: bfloat16 [128, 8, 3, 49], P('lat'), may hold values from -1.5 to 1.5
- lon_reach: int32 [128], P('lat'), may hold values from 1 to 24, as said below
- lat_reach: int32 [128], P('lat'), may hold values from 0 to 1, as said below
Outputs:
- output: bfloat16 [128, 384, 256], P('lat', 'lon')
- grad_in: bfloat16 [128, 384, 256], P('lat', 'lon')
- grad_weight: float32 [2048, 256], P(('lat', 'lon'))
The draws below stay inside these ranges and needn't reach their ends.
Inputs may be any that keep to these rules, and one draw needn't show every extreme that they name: `lon_reach`: reaches widen toward the two poles; the cycles nearest the poles reach 24. `lat_reach`: the first and the last cycle of every aligned block of 16 cycles reach 1.
All inputs are finite; a program needn't handle non-finite values.
Results may differ from the reference program's by a relative error of at most 0.0049.
Values may be sent and summed in bfloat16 or wider, within the bound.
A program may use at most 192 MiB of HBM per device.

```python
import jax
import jax.numpy as jnp
from jax import lax

C = 256
K = 8
ROWS_DEV = 16
REACH = 24
TAPS = 49
KC = 2048
NLAT = 128
NLON = 384


def draw_lon_reach(key, part):
    cycle_ids = jnp.arange(NLAT, dtype=jnp.int32)
    pole_gap = jnp.minimum(cycle_ids, NLAT - 1 - cycle_ids)
    base_reach = 1 + REACH * 4 // (4 + pole_gap)
    jitter = jax.random.randint(jax.random.fold_in(key, 11), (NLAT,), 0, 3)
    return jnp.clip(base_reach + jitter - 1, 1, REACH).astype(jnp.int32)


def draw_lat_reach(key, part):
    cycle_ids = jnp.arange(NLAT, dtype=jnp.int32)
    place = cycle_ids % ROWS_DEV
    at_edge = (place == 0) | (place == ROWS_DEV - 1)
    random_reach = jax.random.randint(jax.random.fold_in(key, 23), (NLAT,), 0, 2)
    return jnp.where(at_edge, 1, random_reach).astype(jnp.int32)


def level_of(own_key, dims, cuts, smallest, top_value):
    def one(position, blocks):
        heights = jax.random.uniform(jax.random.fold_in(jax.random.fold_in(own_key, 6), position), (blocks,), jnp.float32, smallest / len(cuts), top_value / len(cuts))
        return jnp.repeat(jnp.exp(heights), dims[position] // blocks).reshape((-1,) + (1,) * (len(dims) - position - 1))

    level = one(*cuts[0])
    for cut in cuts[1:]:
        level = level * one(*cut)
    return level


def scatter_about(key, extent, width, reach, shards=(), kind=jnp.bfloat16):
    entries = width * jax.random.normal(key, extent, jnp.float32)
    if shards:
        entries = entries * level_of(key, extent, shards, -0.22, 0.18)
    return jnp.clip(entries, -reach, reach).astype(kind)


def setup_inputs(seed: int = 0) -> dict:
    seeds = jax.random.split(jax.random.key(seed), 8)
    return {
        "x_fwd": scatter_about(seeds[0], (NLAT, NLON, C), 1.0, 6.0, ((0, 8), (1, 4))),
        "x_prev": scatter_about(seeds[1], (NLAT, NLON, C), 1.0, 6.0, ((0, 8), (1, 4))),
        "grad_out": scatter_about(seeds[2], (NLAT, NLON, C), 1.0, 6.0, ((0, 8), (1, 4))),
        "weight": scatter_about(seeds[3], (KC, C), KC ** -0.5, 0.125),
        "basis": scatter_about(seeds[4], (NLAT, K, 3, TAPS), 0.25, 1.5, ((0, 8),)),
        "lon_reach": draw_lon_reach(jax.random.fold_in(seeds[7], 71), 0),
        "lat_reach": draw_lat_reach(jax.random.fold_in(seeds[7], 71), 0),
    }


def tap_filters(basis, lon_reach, lat_reach):
    lat_taps = jnp.arange(3, dtype=jnp.int32)
    lon_taps = jnp.arange(TAPS, dtype=jnp.int32)
    live_taps = (jnp.abs(lat_taps - 1)[None, :, None] <= lat_reach[:, None, None]) & (jnp.abs(lon_taps - REACH)[None, None, :] <= lon_reach[:, None, None])
    return jnp.where(live_taps[:, None, :, :], basis, jnp.zeros_like(basis))


def cycle_pad(source):
    cycle = jnp.concatenate([source[:, NLON - REACH:], source, source[:, :REACH]], axis=1)
    return jnp.pad(cycle, ((1, 1), (0, 0), (0, 0)))


def conv_row(padded, filter_row, row_id):
    window = lax.dynamic_slice_in_dim(padded, row_id, 3, 0).astype(jnp.float32)
    stacked = jnp.stack([window[:, shift_col:shift_col + NLON] for shift_col in range(TAPS)], axis=1)
    conv = jnp.einsum('kab,ablc->lkc', filter_row.astype(jnp.float32), stacked)
    return conv.reshape(NLON, KC).astype(jnp.bfloat16)


def spread_row(grad_conv, filter_row):
    grads = grad_conv.astype(jnp.float32).reshape(NLON, K, C)
    cycle = jnp.concatenate([grads[NLON - REACH:], grads, grads[:REACH]], axis=0)
    stacked = jnp.stack([cycle[2 * REACH - shift_col:2 * REACH - shift_col + NLON] for shift_col in range(TAPS)], axis=0)
    return jnp.einsum('kab,blkc->alc', filter_row.astype(jnp.float32), stacked)


def reference(x_fwd, x_prev, grad_out, weight, basis, lon_reach, lat_reach):
    filters = tap_filters(basis, lon_reach, lat_reach)
    pad_fwd = cycle_pad(x_fwd)
    pad_prev = cycle_pad(x_prev)
    row_ids = jnp.arange(NLAT, dtype=jnp.int32)

    def forward_row(row_id):
        filter_row = lax.dynamic_index_in_dim(filters, row_id, 0, keepdims=False)
        conv = conv_row(pad_fwd, filter_row, row_id)
        return jnp.dot(conv, weight, preferred_element_type=jnp.float32).astype(jnp.bfloat16)

    output = lax.map(forward_row, row_ids)

    def backward_row(carry, row_id):
        weight_sum, pending, pending_next = carry
        filter_row = lax.dynamic_index_in_dim(filters, row_id, 0, keepdims=False)
        conv = conv_row(pad_prev, filter_row, row_id)
        grad_row = lax.dynamic_index_in_dim(grad_out, row_id, 0, keepdims=False)
        weight_sum = weight_sum + lax.dot_general(conv, grad_row, (((0,), (0,)), ((), ())), preferred_element_type=jnp.float32)
        grad_conv = lax.dot_general(grad_row, weight, (((1,), (1,)), ((), ())), preferred_element_type=jnp.float32).astype(jnp.bfloat16)
        pieces = spread_row(grad_conv, filter_row)
        finished = pending + pieces[0]
        return (weight_sum, pending_next + pieces[1], pieces[2]), finished

    start_carry = (jnp.zeros((KC, C), jnp.float32), jnp.zeros((NLON, C), jnp.float32), jnp.zeros((NLON, C), jnp.float32))
    final_carry, finished = lax.scan(backward_row, start_carry, row_ids)
    grad_weight, pending, leftover = final_carry
    grad_in = jnp.concatenate([finished[1:], pending[None]], axis=0).astype(jnp.bfloat16)
    return output, grad_in, grad_weight
```

```python
import functools

import jax
import jax.numpy as jnp
from jax import lax
from jax.experimental import pallas as pl
from jax.experimental.pallas import tpu as pltpu
from jax.sharding import PartitionSpec as P


def shifted(value, axis, steps, periodic):
    count = lax.axis_size(axis)
    if periodic:
        pairs = [(source, (source + steps) % count) for source in range(count)]
    else:
        first, last = max(0, -steps), min(count, count - steps)
        pairs = [(source, source + steps) for source in range(first, last)]
    return lax.ppermute(value, axis, pairs)


def edges(block, low, high, reach):
    west = jnp.concatenate([low[None, :reach], block[:, :reach], high[None, :reach]], axis=0)
    east = jnp.concatenate([low[None, -reach:], block[:, -reach:], high[None, -reach:]], axis=0)
    from_west = shifted(east, "lon", 1, True)
    from_east = shifted(west, "lon", -1, True)
    return from_west, from_east


def tap_lanes(filters, span, lanes):
    rows, count, lat_taps, taps = filters.shape
    wide = jnp.pad(filters, ((0, 0), (0, 0), (0, 0), (0, span - taps)))
    wide = wide.reshape(rows, count, lat_taps * span)
    wide = jnp.pad(wide, ((0, 0), (0, 0), (0, lanes - lat_taps * span)))
    return wide.astype(jnp.float32)


def assemble(dest, own, low, high, west, east, reach):
    rows, cols, _ = own.shape
    span = cols + 2 * reach
    for row in range(rows + 2):
        start = row * span
        dest[start : start + reach, :] = west[row]
        dest[start + reach + cols : start + span, :] = east[row]
        if row == 0:
            dest[start + reach : start + reach + cols, :] = low[...]
        elif row == rows + 1:
            dest[start + reach : start + reach + cols, :] = high[...]
        else:
            dest[start + reach : start + reach + cols, :] = own[row - 1]
    tail = dest.shape[0] - (rows + 2) * span
    dest[(rows + 2) * span :, :] = jnp.zeros((tail, dest.shape[1]), dest.dtype)


def build(base, row, dest, cols):
    count, lanes = base.shape[1:]
    taps = base[row]
    for k in range(count):
        start = jnp.broadcast_to(taps[k : k + 1, :], (16, lanes))
        start = pltpu.roll(start, 0, 1, stride=1, stride_axis=0)
        for step in range(cols // 16):
            block = start if step == 0 else pltpu.roll(start, 16 * step, 1)
            dest[k * cols + step * 16 : k * cols + (step + 1) * 16, :] = block.astype(dest.dtype)


def convolve(toeplitz, field, row, span, conv, slot, cols, count):
    chans = field.shape[1]
    begin = pl.multiple_of(row * span, 16)
    window = field[pl.ds(begin, toeplitz.shape[1]), :]
    result = jnp.dot(toeplitz[...], window, preferred_element_type=jnp.float32)
    result = result.astype(jnp.bfloat16)
    place = pl.ds(pl.multiple_of(slot * cols, 16), cols)
    for k in range(count):
        conv[place, k * chans : (k + 1) * chans] = result[k * cols : (k + 1) * cols, :]


def weight_kernel(group, reach, base, own, low, high, west, east, grad, out, field, toeplitz, conv, total):
    step = pl.program_id(0)
    rows, cols, chans = own.shape
    count = base.shape[1]
    span = cols + 2 * reach

    @pl.when(step == 0)
    def _():
        assemble(field, own, low, high, west, east, reach)
        total[...] = jnp.zeros_like(total)

    def one(slot, carry):
        row = step * group + slot
        build(base, row, toeplitz, cols)
        convolve(toeplitz, field, row, span, conv, slot, cols, count)
        return carry

    lax.fori_loop(0, group, one, 0)
    cotangent = grad[...].reshape(group * cols, chans)
    total[...] += lax.dot_general(
        cotangent, conv[...], (((0,), (0,)), ((), ())), preferred_element_type=jnp.float32
    )

    @pl.when(step == pl.num_programs(0) - 1)
    def _():
        for k in range(count):
            out[k * chans : (k + 1) * chans, :] = total[:, k * chans : (k + 1) * chans].T.astype(out.dtype)


def field_kernel(group, reach, base, base_back, f_own, f_low, f_high, f_west, f_east, g_own, g_low, g_high, g_west, g_east, weight, weight_back, out, grad_in, f_field, g_field, toeplitz, toeplitz_back, f_conv, g_conv):
    step = pl.program_id(0)
    rows, cols, chans = f_own.shape
    count = base.shape[1]
    span = cols + 2 * reach

    @pl.when(step == 0)
    def _():
        assemble(f_field, f_own, f_low, f_high, f_west, f_east, reach)
        assemble(g_field, g_own, g_low, g_high, g_west, g_east, reach)

    def one(slot, carry):
        row = step * group + slot
        build(base, row, toeplitz, cols)
        build(base_back, row, toeplitz_back, cols)
        convolve(toeplitz, f_field, row, span, f_conv, slot, cols, count)
        convolve(toeplitz_back, g_field, row, span, g_conv, slot, cols, count)
        return carry

    lax.fori_loop(0, group, one, 0)
    mixed = jnp.dot(f_conv[...], weight[...], preferred_element_type=jnp.float32)
    out[...] = mixed.astype(out.dtype).reshape(out.shape)
    mixed = jnp.dot(g_conv[...], weight_back[...], preferred_element_type=jnp.float32)
    grad_in[...] = mixed.astype(grad_in.dtype).reshape(grad_in.shape)


def whole(array):
    rank = array.ndim
    return pl.BlockSpec(array.shape, lambda i: (0,) * rank)


def local(x_fwd, x_prev, grad_out, weight, basis, lon_reach, lat_reach):
    rows, cols, chans = x_fwd.shape
    _, count, lat_count, taps = basis.shape
    reach = (taps - 1) // 2
    span = cols + 2 * reach
    lanes = -(-lat_count * span // 256) * 256
    height = (rows - 1) * span + lanes
    height = max(height, (rows + 2) * span)
    group = 4 if rows % 4 == 0 else 1
    lat_taps = jnp.arange(lat_count, dtype=jnp.int32)
    lon_taps = jnp.arange(taps, dtype=jnp.int32)
    live = (jnp.abs(lat_taps - 1)[None, :, None] <= lat_reach[:, None, None]) & (
        jnp.abs(lon_taps - reach)[None, None, :] <= lon_reach[:, None, None]
    )
    filters = jnp.where(live[:, None, :, :], basis, jnp.zeros_like(basis))

    tiles = jnp.pad(
        filters[jnp.array([0, rows - 1])].reshape(2, count * lat_count, taps),
        ((0, 0), (0, 0), (0, chans - taps)),
    )
    prev_low = shifted(x_prev[-1], "lat", 1, False)
    prev_high = shifted(x_prev[0], "lat", -1, False)
    up = jnp.concatenate([x_fwd[-1], grad_out[-1], tiles[1]], axis=0)
    down = jnp.concatenate([x_fwd[0], grad_out[0], tiles[0]], axis=0)
    up = shifted(up, "lat", 1, False)
    down = shifted(down, "lat", -1, False)
    f_low, g_low, tile_low = up[:cols], up[cols : 2 * cols], up[2 * cols :, :taps]
    f_high, g_high, tile_high = down[:cols], down[cols : 2 * cols], down[2 * cols :, :taps]
    p_west, p_east = edges(x_prev, prev_low, prev_high, reach)
    f_west, f_east = edges(x_fwd, f_low, f_high, reach)
    g_west, g_east = edges(grad_out, g_low, g_high, reach)

    shape = (1, count, lat_count, taps)
    tall = jnp.concatenate([tile_low.reshape(shape), filters, tile_high.reshape(shape)], axis=0)
    flipped = tall[:, :, :, ::-1]
    back = jnp.stack(
        [flipped[a : a + rows, :, lat_count - 1 - a] for a in range(lat_count)], axis=2
    )
    base = tap_lanes(filters, span, lanes)
    base_back = tap_lanes(back, span, lanes)
    weight_back = weight.reshape(count, chans, chans).transpose(0, 2, 1).reshape(weight.shape)

    steps = rows // group
    limit = 60 * 1024 * 1024
    conv_flops = 2 * rows * count * cols * lanes * chans
    mix_flops = 2 * rows * cols * count * chans * chans
    blocked = pl.BlockSpec((group, cols, chans), lambda i: (i, 0, 0))
    operands = (base, x_prev, prev_low, prev_high, p_west, p_east)
    term = pl.pallas_call(
        functools.partial(weight_kernel, group, reach),
        grid=(steps,),
        in_specs=[whole(a) for a in operands] + [blocked],
        out_specs=pl.BlockSpec(weight.shape, lambda i: (0, 0)),
        out_shape=jax.ShapeDtypeStruct(weight.shape, jnp.bfloat16),
        scratch_shapes=[
            pltpu.VMEM((height, chans), jnp.bfloat16),
            pltpu.VMEM((count * cols, lanes), jnp.bfloat16),
            pltpu.VMEM((group * cols, count * chans), jnp.bfloat16),
            pltpu.VMEM((chans, count * chans), jnp.float32),
        ],
        compiler_params=pltpu.CompilerParams(vmem_limit_bytes=limit),
        cost_estimate=pl.CostEstimate(flops=conv_flops + mix_flops, bytes_accessed=4 << 20, transcendentals=0),
    )(*operands, grad_out)

    devices = lax.axis_size("lat") * lax.axis_size("lon")
    pieces = lax.all_to_all(
        term.reshape(devices, weight.shape[0] // devices, chans), ("lat", "lon"), 0, 0
    )

    operands = (base, base_back, x_fwd, f_low, f_high, f_west, f_east, grad_out, g_low, g_high, g_west, g_east, weight, weight_back)
    output, grad_in = pl.pallas_call(
        functools.partial(field_kernel, group, reach),
        grid=(steps,),
        in_specs=[whole(a) for a in operands],
        out_specs=[blocked, blocked],
        out_shape=[jax.ShapeDtypeStruct(x_fwd.shape, jnp.bfloat16)] * 2,
        scratch_shapes=[
            pltpu.VMEM((height, chans), jnp.bfloat16),
            pltpu.VMEM((height, chans), jnp.bfloat16),
            pltpu.VMEM((count * cols, lanes), jnp.bfloat16),
            pltpu.VMEM((count * cols, lanes), jnp.bfloat16),
            pltpu.VMEM((group * cols, count * chans), jnp.bfloat16),
            pltpu.VMEM((group * cols, count * chans), jnp.bfloat16),
        ],
        compiler_params=pltpu.CompilerParams(vmem_limit_bytes=limit),
        cost_estimate=pl.CostEstimate(flops=2 * (conv_flops + mix_flops), bytes_accessed=8 << 20, transcendentals=0),
    )(*operands)
    grad_weight = jnp.sum(pieces.astype(jnp.float32), axis=0)
    return output, grad_in, grad_weight


def solution(mesh):
    return jax.shard_map(
        local,
        mesh=mesh,
        in_specs=(
            P("lat", "lon", None),
            P("lat", "lon", None),
            P("lat", "lon", None),
            P(),
            P("lat", None, None, None),
            P("lat"),
            P("lat"),
        ),
        out_specs=(P("lat", "lon", None), P("lat", "lon", None), P(("lat", "lon"), None)),
        check_vma=False,
    )
```

```python
import functools

import jax
import jax.numpy as jnp
from jax import lax
from jax.experimental import pallas as pl
from jax.experimental.pallas import tpu as pltpu
from jax.sharding import PartitionSpec as P


MESH = pl.DeviceIdType.MESH


def tap_lanes(taps, span, lanes):
    rows, count, lat_taps, width = taps.shape
    wide = jnp.pad(taps, ((0, 0), (0, 0), (0, 0), (0, span - width)))
    wide = wide.reshape(rows, count, lat_taps * span)
    return jnp.pad(wide, ((0, 0), (0, 0), (0, lanes - lat_taps * span)))


def halo_copies(own, low, high, west, east, reach, send, recv, first):
    rows, cols, _ = own.shape
    lat, lon = lax.axis_index("lat"), lax.axis_index("lon")
    lats, lons = lax.axis_size("lat"), lax.axis_size("lon")
    up, down = lax.rem(lat + 1, lats), lax.rem(lat + lats - 1, lats)
    right, left = lax.rem(lon + 1, lons), lax.rem(lon + lons - 1, lons)
    east_edge, west_edge = pl.ds(cols - reach, reach), pl.ds(0, reach)
    moves = (
        (own.at[:, east_edge], west.at[pl.ds(1, rows)], lat, right),
        (own.at[:, west_edge], east.at[pl.ds(1, rows)], lat, left),
        (own.at[rows - 1], low, up, lon),
        (own.at[0], high, down, lon),
        (own.at[rows - 1, east_edge], west.at[0], up, right),
        (own.at[rows - 1, west_edge], east.at[0], up, left),
        (own.at[0, east_edge], west.at[rows + 1], down, right),
        (own.at[0, west_edge], east.at[rows + 1], down, left),
    )
    return [
        pltpu.make_async_remote_copy(
            src_ref=source,
            dst_ref=target,
            send_sem=send.at[first + n],
            recv_sem=recv.at[first + n],
            device_id={"lat": lat_id, "lon": lon_id},
            device_id_type=MESH,
        )
        for n, (source, target, lat_id, lon_id) in enumerate(moves)
    ]


def assemble(dest, own, low, high, west, east, reach):
    rows, cols, _ = own.shape
    span = cols + 2 * reach
    for row in range(rows + 2):
        start = row * span
        dest[start : start + reach, :] = west[row]
        dest[start + reach + cols : start + span, :] = east[row]
        if row == 0:
            dest[start + reach : start + reach + cols, :] = low[...]
        elif row == rows + 1:
            dest[start + reach : start + reach + cols, :] = high[...]
        else:
            dest[start + reach : start + reach + cols, :] = own[row - 1]
    tail = dest.shape[0] - (rows + 2) * span
    dest[(rows + 2) * span :, :] = jnp.zeros((tail, dest.shape[1]), dest.dtype)


def build(taps, dest, cols):
    count, lanes = taps.shape
    for k in range(count):
        start = jnp.broadcast_to(taps[k : k + 1, :], (16, lanes))
        start = pltpu.roll(start, 0, 1, stride=1, stride_axis=0)
        for step in range(cols // 16):
            block = start if step == 0 else pltpu.roll(start, 16 * step, 1)
            dest[k * cols + step * 16 : k * cols + (step + 1) * 16, :] = block.astype(dest.dtype)


def convolve(toeplitz, field, row, span, conv, slot, cols, count):
    chans = field.shape[1]
    begin = pl.multiple_of(row * span, 16)
    window = field[pl.ds(begin, toeplitz.shape[1]), :]
    result = jnp.dot(toeplitz[...], window, preferred_element_type=jnp.float32)
    result = result.astype(jnp.bfloat16)
    place = pl.ds(pl.multiple_of(slot * cols, 16), cols)
    for k in range(count):
        conv[place, k * chans : (k + 1) * chans] = result[k * cols : (k + 1) * cols, :]


def weight_kernel(group, reach, base, back, own, f_own, g_own, g_hbm, term, f_low, f_high, f_west, f_east, g_low, g_high, g_west, g_east, b_low, b_high, low, high, west, east, q_low, q_high, field, even, odd, conv, total, send, recv):
    rows, cols, chans = own.shape
    count = base.shape[1]
    span = cols + 2 * reach
    lat, lon = lax.axis_index("lat"), lax.axis_index("lon")
    lats, lons = lax.axis_size("lat"), lax.axis_size("lon")
    barrier = pltpu.get_barrier_semaphore()
    for lat_move in (1, 0, lats - 1):
        for lon_move in (1, 0, lons - 1):
            if lat_move or lon_move:
                pl.semaphore_signal(
                    barrier,
                    inc=1,
                    device_id={"lat": lax.rem(lat + lat_move, lats), "lon": lax.rem(lon + lon_move, lons)},
                    device_id_type=MESH,
                )
    pl.semaphore_wait(barrier, 8)
    now = halo_copies(own, low, high, west, east, reach, send, recv, 0)
    later = halo_copies(f_own, f_low, f_high, f_west, f_east, reach, send, recv, 8)
    later += halo_copies(g_hbm, g_low, g_high, g_west, g_east, reach, send, recv, 16)
    for n, (source, target, move) in enumerate(((rows - 1, q_low, 1), (0, q_high, lats - 1))):
        later.append(
            pltpu.make_async_remote_copy(
                src_ref=back.at[source],
                dst_ref=target,
                send_sem=send.at[24 + n],
                recv_sem=recv.at[24 + n],
                device_id={"lat": lax.rem(lat + move, lats), "lon": lon},
                device_id_type=MESH,
            )
        )
    for copy in now + later:
        copy.start()
    build(base[0], even, cols)
    total[...] = jnp.zeros_like(total)
    for copy in now:
        copy.wait()
    assemble(field, own, low, high, west, east, reach)

    def pair(number, carry):
        row = number * 2
        slot = lax.rem(row, group)
        build(base[row + 1], odd, cols)
        convolve(even, field, row, span, conv, slot, cols, count)
        build(base[lax.rem(row + 2, rows)], even, cols)
        convolve(odd, field, row + 1, span, conv, slot + 1, cols, count)
        return carry

    def several(step, carry):
        lax.fori_loop(step * (group // 2), (step + 1) * (group // 2), pair, 0)
        cotangent = g_own[pl.ds(step * group, group)].reshape(group * cols, chans)
        total[...] += lax.dot_general(
            cotangent, conv[...], (((0,), (0,)), ((), ())), preferred_element_type=jnp.float32
        )
        return carry

    lax.fori_loop(0, rows // group, several, 0)
    for k in range(count):
        term[k * chans : (k + 1) * chans, :] = total[:, k * chans : (k + 1) * chans].T.astype(term.dtype)
    for copy in later:
        copy.wait()
    b_low[...] = jnp.where(lat == 0, jnp.zeros_like(b_low), q_low[...])
    b_high[...] = jnp.where(lat == lats - 1, jnp.zeros_like(b_high), q_high[...])


def field_kernel(group, reach, base, back, b_low, b_high, f_own, f_low, f_high, f_west, f_east, g_own, g_low, g_high, g_west, g_east, weight, weight_back, out, grad_in, f_field, g_field, taps, f_even, f_odd, g_even, g_odd, f_conv, g_conv):
    step = pl.program_id(0)
    rows, cols, chans = f_own.shape
    count, lanes = base.shape[1:]
    span = cols + 2 * reach
    lane = lax.broadcasted_iota(jnp.int32, (count, lanes), 1)

    def back_taps(row):
        return jnp.where(lane < span, taps[row], jnp.where(lane < 2 * span, taps[row + 1], taps[row + 2]))

    @pl.when(step == 0)
    def _():
        assemble(f_field, f_own, f_low, f_high, f_west, f_east, reach)
        assemble(g_field, g_own, g_low, g_high, g_west, g_east, reach)
        taps[0] = b_low[...]
        taps[pl.ds(1, rows)] = back[...]
        taps[rows + 1] = b_high[...]
        build(base[0], f_even, cols)
        build(back_taps(0), g_even, cols)

    def pair(number, carry):
        slot = number * 2
        row = step * group + slot
        follow = lax.rem(row + 2, rows)
        build(base[row + 1], f_odd, cols)
        convolve(f_even, f_field, row, span, f_conv, slot, cols, count)
        build(back_taps(row + 1), g_odd, cols)
        convolve(g_even, g_field, row, span, g_conv, slot, cols, count)
        build(base[follow], f_even, cols)
        convolve(f_odd, f_field, row + 1, span, f_conv, slot + 1, cols, count)
        build(back_taps(follow), g_even, cols)
        convolve(g_odd, g_field, row + 1, span, g_conv, slot + 1, cols, count)
        return carry

    lax.fori_loop(0, group // 2, pair, 0)
    mixed = jnp.dot(f_conv[...], weight[...], preferred_element_type=jnp.float32)
    out[...] = mixed.astype(out.dtype).reshape(out.shape)
    mixed = jnp.dot(g_conv[...], weight_back[...], preferred_element_type=jnp.float32)
    grad_in[...] = mixed.astype(grad_in.dtype).reshape(grad_in.shape)


def whole(array):
    rank = array.ndim
    return pl.BlockSpec(array.shape, lambda i: (0,) * rank)


def local(x_fwd, x_prev, grad_out, weight, basis, lon_reach, lat_reach):
    rows, cols, chans = x_fwd.shape
    _, count, lat_count, taps = basis.shape
    reach = (taps - 1) // 2
    span = cols + 2 * reach
    lanes = -(-lat_count * span // 256) * 256
    height = (rows - 1) * span + lanes
    height = max(height, (rows + 2) * span)
    group = 4 if rows % 4 == 0 else 2
    lats = lax.axis_size("lat")
    place = jnp.arange(lanes, dtype=jnp.int32)
    lat_tap, lon_tap = place // span, place % span
    row_ids = lax.axis_index("lat") * rows + jnp.arange(rows, dtype=jnp.int32)
    live = (jnp.abs(lat_tap - 1)[None, :] <= lat_reach[:, None]) & (
        jnp.abs(lon_tap - reach)[None, :] <= lon_reach[:, None]
    )
    source = row_ids[:, None] + lat_tap[None, :] - 1
    inside = live & (source >= 0) & (source < rows * lats)
    base = tap_lanes(basis, span, lanes)
    base = jnp.where(inside[:, None, :], base, jnp.zeros_like(base)).astype(jnp.float32)
    back = tap_lanes(basis[:, :, ::-1, ::-1], span, lanes)
    back = jnp.where(live[:, None, :], back, jnp.zeros_like(back)).astype(jnp.float32)
    weight_back = weight.reshape(count, chans, chans).transpose(0, 2, 1).reshape(weight.shape)

    steps = rows // group
    limit = 60 * 1024 * 1024
    conv_flops = 2 * rows * count * cols * lanes * chans
    mix_flops = 2 * rows * cols * count * chans * chans
    blocked = pl.BlockSpec((group, cols, chans), lambda i: (i, 0, 0))
    vmem, anywhere = pl.BlockSpec(memory_space=pltpu.VMEM), pl.BlockSpec(memory_space=pl.ANY)
    line = jax.ShapeDtypeStruct((cols, chans), jnp.bfloat16)
    side = jax.ShapeDtypeStruct((rows + 2, reach, chans), jnp.bfloat16)
    tile = jax.ShapeDtypeStruct((count, lanes), jnp.float32)
    band = pltpu.VMEM((height, chans), jnp.bfloat16)
    square = pltpu.VMEM((count * cols, lanes), jnp.bfloat16)
    wide = pltpu.VMEM((group * cols, count * chans), jnp.bfloat16)
    term, f_low, f_high, f_west, f_east, g_low, g_high, g_west, g_east, b_low, b_high = pl.pallas_call(
        functools.partial(weight_kernel, group, reach),
        in_specs=[vmem, anywhere, vmem, anywhere, vmem, anywhere],
        out_specs=[vmem] + [anywhere] * 8 + [vmem] * 2,
        out_shape=[jax.ShapeDtypeStruct(weight.shape, jnp.bfloat16)] + [line, line, side, side] * 2 + [tile] * 2,
        scratch_shapes=[
            pltpu.VMEM(line.shape, line.dtype),
            pltpu.VMEM(line.shape, line.dtype),
            pltpu.VMEM(side.shape, side.dtype),
            pltpu.VMEM(side.shape, side.dtype),
            pltpu.VMEM(tile.shape, tile.dtype),
            pltpu.VMEM(tile.shape, tile.dtype),
            band,
            square,
            square,
            wide,
            pltpu.VMEM((chans, count * chans), jnp.float32),
            pltpu.SemaphoreType.DMA((26,)),
            pltpu.SemaphoreType.DMA((26,)),
        ],
        compiler_params=pltpu.CompilerParams(vmem_limit_bytes=limit, collective_id=0, has_side_effects=True),
        cost_estimate=pl.CostEstimate(flops=conv_flops + mix_flops, bytes_accessed=4 << 20, transcendentals=0),
    )(base, back, x_prev, x_fwd, grad_out, grad_out)

    devices = lax.axis_size("lat") * lax.axis_size("lon")
    pieces = lax.all_to_all(
        term.reshape(devices, weight.shape[0] // devices, chans), ("lat", "lon"), 0, 0
    )

    operands = (base, back, b_low, b_high, x_fwd, f_low, f_high, f_west, f_east, grad_out, g_low, g_high, g_west, g_east, weight, weight_back)
    output, grad_in = pl.pallas_call(
        functools.partial(field_kernel, group, reach),
        grid=(steps,),
        in_specs=[whole(a) for a in operands],
        out_specs=[blocked, blocked],
        out_shape=[jax.ShapeDtypeStruct(x_fwd.shape, jnp.bfloat16)] * 2,
        scratch_shapes=[band, band, pltpu.VMEM((rows + 2, count, lanes), jnp.float32)]
        + [square] * 4
        + [wide] * 2,
        compiler_params=pltpu.CompilerParams(vmem_limit_bytes=limit),
        cost_estimate=pl.CostEstimate(flops=2 * (conv_flops + mix_flops), bytes_accessed=8 << 20, transcendentals=0),
    )(*operands)
    grad_weight = jnp.sum(pieces.astype(jnp.float32), axis=0)
    return output, grad_in, grad_weight


def solution(mesh):
    return jax.shard_map(
        local,
        mesh=mesh,
        in_specs=(
            P("lat", "lon", None),
            P("lat", "lon", None),
            P("lat", "lon", None),
            P(),
            P("lat", None, None, None),
            P("lat"),
            P("lat"),
        ),
        out_specs=(P("lat", "lon", None), P("lat", "lon", None), P(("lat", "lon"), None)),
        check_vma=False,
    )
```

```python
import functools

import jax
import jax.numpy as jnp
from jax import lax
from jax.experimental import pallas as pl
from jax.experimental.pallas import tpu as pltpu
from jax.sharding import PartitionSpec as P


MESH = pl.DeviceIdType.MESH


def tap_lanes(taps, span, lanes):
    rows, count, lat_taps, width = taps.shape
    wide = jnp.pad(taps, ((0, 0), (0, 0), (0, 0), (0, span - width)))
    wide = wide.reshape(rows, count, lat_taps * span)
    return jnp.pad(wide, ((0, 0), (0, 0), (0, lanes - lat_taps * span)))


def halo_copies(own, low, high, west, east, reach, send, recv, first):
    rows, cols, _ = own.shape
    lat, lon = lax.axis_index("lat"), lax.axis_index("lon")
    lats, lons = lax.axis_size("lat"), lax.axis_size("lon")
    up, down = lax.rem(lat + 1, lats), lax.rem(lat + lats - 1, lats)
    right, left = lax.rem(lon + 1, lons), lax.rem(lon + lons - 1, lons)
    east_edge, west_edge = pl.ds(cols - reach, reach), pl.ds(0, reach)
    moves = (
        (own.at[:, east_edge], west.at[pl.ds(1, rows)], lat, right),
        (own.at[:, west_edge], east.at[pl.ds(1, rows)], lat, left),
        (own.at[rows - 1], low, up, lon),
        (own.at[0], high, down, lon),
        (own.at[rows - 1, east_edge], west.at[0], up, right),
        (own.at[rows - 1, west_edge], east.at[0], up, left),
        (own.at[0, east_edge], west.at[rows + 1], down, right),
        (own.at[0, west_edge], east.at[rows + 1], down, left),
    )
    return [
        pltpu.make_async_remote_copy(
            src_ref=source,
            dst_ref=target,
            send_sem=send.at[first + n],
            recv_sem=recv.at[first + n],
            device_id={"lat": lat_id, "lon": lon_id},
            device_id_type=MESH,
        )
        for n, (source, target, lat_id, lon_id) in enumerate(moves)
    ]


def assemble(dest, own, low, high, west, east, reach):
    rows, cols, _ = own.shape
    span = cols + 2 * reach
    for row in range(rows + 2):
        start = row * span
        dest[start : start + reach, :] = west[row]
        dest[start + reach + cols : start + span, :] = east[row]
        if row == 0:
            dest[start + reach : start + reach + cols, :] = low[...]
        elif row == rows + 1:
            dest[start + reach : start + reach + cols, :] = high[...]
        else:
            dest[start + reach : start + reach + cols, :] = own[row - 1]
    tail = dest.shape[0] - (rows + 2) * span
    dest[(rows + 2) * span :, :] = jnp.zeros((tail, dest.shape[1]), dest.dtype)


def build(taps, dest, cols):
    count, lanes = taps.shape
    for k in range(count):
        start = jnp.broadcast_to(taps[k : k + 1, :], (16, lanes))
        start = pltpu.roll(start, 0, 1, stride=1, stride_axis=0).astype(dest.dtype)
        for step in range(cols // 16):
            block = start if step == 0 else pltpu.roll(start, 16 * step, 1)
            dest[k * cols + step * 16 : k * cols + (step + 1) * 16, :] = block


def convolve(toeplitz, field, row, span, conv, slot, cols, count):
    chans = field.shape[1]
    begin = pl.multiple_of(row * span, 16)
    window = field[pl.ds(begin, toeplitz.shape[1]), :]
    result = jnp.dot(toeplitz[...], window, preferred_element_type=jnp.float32)
    result = result.astype(jnp.bfloat16)
    place = slice(slot * cols, (slot + 1) * cols)
    for k in range(count):
        conv[place, k * chans : (k + 1) * chans] = result[k * cols : (k + 1) * cols, :]


def weight_kernel(group, reach, base, back, own, f_own, g_own, g_hbm, term, f_low, f_high, f_west, f_east, g_low, g_high, g_west, g_east, b_low, b_high, low, high, west, east, q_low, q_high, field, even, odd, conv, total, send, recv):
    rows, cols, chans = own.shape
    count = base.shape[1]
    span = cols + 2 * reach
    lat, lon = lax.axis_index("lat"), lax.axis_index("lon")
    lats, lons = lax.axis_size("lat"), lax.axis_size("lon")
    barrier = pltpu.get_barrier_semaphore()
    for lat_move in (1, 0, lats - 1):
        for lon_move in (1, 0, lons - 1):
            if lat_move or lon_move:
                pl.semaphore_signal(
                    barrier,
                    inc=1,
                    device_id={"lat": lax.rem(lat + lat_move, lats), "lon": lax.rem(lon + lon_move, lons)},
                    device_id_type=MESH,
                )
    pl.semaphore_wait(barrier, 8)
    now = halo_copies(own, low, high, west, east, reach, send, recv, 0)
    later = halo_copies(f_own, f_low, f_high, f_west, f_east, reach, send, recv, 8)
    later += halo_copies(g_hbm, g_low, g_high, g_west, g_east, reach, send, recv, 16)
    for n, (source, target, move) in enumerate(((rows - 1, q_low, 1), (0, q_high, lats - 1))):
        later.append(
            pltpu.make_async_remote_copy(
                src_ref=back.at[source],
                dst_ref=target,
                send_sem=send.at[24 + n],
                recv_sem=recv.at[24 + n],
                device_id={"lat": lax.rem(lat + move, lats), "lon": lon},
                device_id_type=MESH,
            )
        )
    for copy in now:
        copy.start()
    total[...] = jnp.zeros_like(total)
    for copy in now:
        copy.wait()
    for copy in later:
        copy.start()
    assemble(field, own, low, high, west, east, reach)

    def several(step, carry):
        for slot in range(group):
            toeplitz = (even, odd)[slot % 2]
            build(base[step * group + slot], toeplitz, cols)
            convolve(toeplitz, field, step * group + slot, span, conv, slot, cols, count)
        cotangent = g_own[pl.ds(step * group, group)].reshape(group * cols, chans)
        total[...] += lax.dot_general(
            cotangent, conv[...], (((0,), (0,)), ((), ())), preferred_element_type=jnp.float32
        )
        return carry

    lax.fori_loop(0, rows // group, several, 0)
    for k in range(count):
        term[k * chans : (k + 1) * chans, :] = total[:, k * chans : (k + 1) * chans].T.astype(term.dtype)
    for copy in later:
        copy.wait()
    b_low[...] = jnp.where(lat == 0, jnp.zeros_like(b_low), q_low[...])
    b_high[...] = jnp.where(lat == lats - 1, jnp.zeros_like(b_high), q_high[...])


def field_kernel(group, reach, base, back, b_low, b_high, f_own, f_low, f_high, f_west, f_east, g_own, g_low, g_high, g_west, g_east, weight, weight_back, out, grad_in, f_field, g_field, taps, f_even, f_odd, g_even, g_odd, f_conv, g_conv):
    step = pl.program_id(0)
    rows, cols, chans = f_own.shape
    count, lanes = base.shape[1:]
    span = cols + 2 * reach
    lane = lax.broadcasted_iota(jnp.int32, (count, lanes), 1)

    def back_taps(row):
        return jnp.where(lane < span, taps[row], jnp.where(lane < 2 * span, taps[row + 1], taps[row + 2]))

    @pl.when(step == 0)
    def _():
        assemble(f_field, f_own, f_low, f_high, f_west, f_east, reach)
        assemble(g_field, g_own, g_low, g_high, g_west, g_east, reach)
        taps[0] = b_low[...]
        taps[pl.ds(1, rows)] = back[...]
        taps[rows + 1] = b_high[...]

    for slot in range(group):
        row = step * group + slot
        f_square, g_square = ((f_even, g_even), (f_odd, g_odd))[slot % 2]
        build(base[row], f_square, cols)
        convolve(f_square, f_field, row, span, f_conv, slot, cols, count)
        build(back_taps(row), g_square, cols)
        convolve(g_square, g_field, row, span, g_conv, slot, cols, count)
    mixed = jnp.dot(f_conv[...], weight[...], preferred_element_type=jnp.float32)
    out[...] = mixed.astype(out.dtype).reshape(out.shape)
    mixed = jnp.dot(g_conv[...], weight_back[...], preferred_element_type=jnp.float32)
    grad_in[...] = mixed.astype(grad_in.dtype).reshape(grad_in.shape)


def whole(array):
    rank = array.ndim
    return pl.BlockSpec(array.shape, lambda i: (0,) * rank)


def local(x_fwd, x_prev, grad_out, weight, basis, lon_reach, lat_reach):
    rows, cols, chans = x_fwd.shape
    _, count, lat_count, taps = basis.shape
    reach = (taps - 1) // 2
    span = cols + 2 * reach
    lanes = -(-lat_count * span // 256) * 256
    height = (rows - 1) * span + lanes
    height = max(height, (rows + 2) * span)
    group = 4 if rows % 4 == 0 else 2
    lats = lax.axis_size("lat")
    place = jnp.arange(lanes, dtype=jnp.int32)
    lat_tap, lon_tap = place // span, place % span
    row_ids = lax.axis_index("lat") * rows + jnp.arange(rows, dtype=jnp.int32)
    live = (jnp.abs(lat_tap - 1)[None, :] <= lat_reach[:, None]) & (
        jnp.abs(lon_tap - reach)[None, :] <= lon_reach[:, None]
    )
    source = row_ids[:, None] + lat_tap[None, :] - 1
    inside = live & (source >= 0) & (source < rows * lats)
    base = tap_lanes(basis, span, lanes)
    base = jnp.where(inside[:, None, :], base, jnp.zeros_like(base)).astype(jnp.float32)
    back = tap_lanes(basis[:, :, ::-1, ::-1], span, lanes)
    back = jnp.where(live[:, None, :], back, jnp.zeros_like(back)).astype(jnp.float32)
    weight_back = weight.reshape(count, chans, chans).transpose(0, 2, 1).reshape(weight.shape)

    steps = rows // group
    limit = 60 * 1024 * 1024
    conv_flops = 2 * rows * count * cols * lanes * chans
    mix_flops = 2 * rows * cols * count * chans * chans
    blocked = pl.BlockSpec((group, cols, chans), lambda i: (i, 0, 0))
    vmem, anywhere = pl.BlockSpec(memory_space=pltpu.VMEM), pl.BlockSpec(memory_space=pl.ANY)
    line = jax.ShapeDtypeStruct((cols, chans), jnp.bfloat16)
    side = jax.ShapeDtypeStruct((rows + 2, reach, chans), jnp.bfloat16)
    tile = jax.ShapeDtypeStruct((count, lanes), jnp.float32)
    band = pltpu.VMEM((height, chans), jnp.bfloat16)
    square = pltpu.VMEM((count * cols, lanes), jnp.bfloat16)
    wide = pltpu.VMEM((group * cols, count * chans), jnp.bfloat16)
    term, f_low, f_high, f_west, f_east, g_low, g_high, g_west, g_east, b_low, b_high = pl.pallas_call(
        functools.partial(weight_kernel, group, reach),
        in_specs=[vmem, anywhere, vmem, anywhere, vmem, anywhere],
        out_specs=[vmem] + [anywhere] * 8 + [vmem] * 2,
        out_shape=[jax.ShapeDtypeStruct(weight.shape, jnp.bfloat16)] + [line, line, side, side] * 2 + [tile] * 2,
        scratch_shapes=[
            pltpu.VMEM(line.shape, line.dtype),
            pltpu.VMEM(line.shape, line.dtype),
            pltpu.VMEM(side.shape, side.dtype),
            pltpu.VMEM(side.shape, side.dtype),
            pltpu.VMEM(tile.shape, tile.dtype),
            pltpu.VMEM(tile.shape, tile.dtype),
            band,
            square,
            square,
            wide,
            pltpu.VMEM((chans, count * chans), jnp.float32),
            pltpu.SemaphoreType.DMA((26,)),
            pltpu.SemaphoreType.DMA((26,)),
        ],
        compiler_params=pltpu.CompilerParams(vmem_limit_bytes=limit, collective_id=0, has_side_effects=True),
        cost_estimate=pl.CostEstimate(flops=conv_flops + mix_flops, bytes_accessed=4 << 20, transcendentals=0),
    )(base, back, x_prev, x_fwd, grad_out, grad_out)

    devices = lax.axis_size("lat") * lax.axis_size("lon")
    pieces = lax.all_to_all(
        term.reshape(devices, weight.shape[0] // devices, chans), ("lat", "lon"), 0, 0
    )

    operands = (base, back, b_low, b_high, x_fwd, f_low, f_high, f_west, f_east, grad_out, g_low, g_high, g_west, g_east, weight, weight_back)
    output, grad_in = pl.pallas_call(
        functools.partial(field_kernel, group, reach),
        grid=(steps,),
        in_specs=[whole(a) for a in operands],
        out_specs=[blocked, blocked],
        out_shape=[jax.ShapeDtypeStruct(x_fwd.shape, jnp.bfloat16)] * 2,
        scratch_shapes=[band, band, pltpu.VMEM((rows + 2, count, lanes), jnp.float32)]
        + [square] * 4
        + [wide] * 2,
        compiler_params=pltpu.CompilerParams(vmem_limit_bytes=limit),
        cost_estimate=pl.CostEstimate(flops=2 * (conv_flops + mix_flops), bytes_accessed=8 << 20, transcendentals=0),
    )(*operands)
    grad_weight = jnp.sum(pieces.astype(jnp.float32), axis=0)
    return output, grad_in, grad_weight


def solution(mesh):
    return jax.shard_map(
        local,
        mesh=mesh,
        in_specs=(
            P("lat", "lon", None),
            P("lat", "lon", None),
            P("lat", "lon", None),
            P(),
            P("lat", None, None, None),
            P("lat"),
            P("lat"),
        ),
        out_specs=(P("lat", "lon", None), P("lat", "lon", None), P(("lat", "lon"), None)),
        check_vma=False,
    )
```
